32 devices in a mesh: gx: 2 (over x), gy: 4 (over y, core), gz: 4 (over z).
Axes of the slice: x: 2, y: 2, z: 4, core: 2. Of those that a mesh axis runs over, the one named last changes fastest.
Arguments:
- field: float32 [448, 448, 448], P(('gx', 'gy'), 'gz'), may hold values from -6 to 6
- forward: float32 [2, 224, 224], replicated, may hold values from -0.375 to 0.375
- inverse: float32 [2, 224, 224], replicated, may hold values from -0.375 to 0.375
- eigen: float32 [448], replicated, may hold values from 0.05 to 20
Outputs:
- solution: float32 [448, 448, 448], P(('gx', 'gy'), 'gz')
The draws below stay inside these ranges and needn't reach their ends.
All inputs are finite; a program needn't handle non-finite values.
Results may differ from the reference program's by a relative error of at most 0.000071.
Values sent between devices are 32-bit elements; how exact they have to be, the bound alone decides.
No kernel may reach another device: no remote copies, remote signals or barrier semaphores. Data moves between devices by JAX's collectives and lax.ppermute only.
A program may use at most 128 MiB of HBM per device.

```python
import math
import jax
import jax.numpy as jnp
from jax import lax

N = 448
HALF = 224


def block_scale(own_key, dims, cuts, low, top_value):
    gain = 1.0
    for axis_at, blocks in cuts:
        steps = jax.random.uniform(jax.random.fold_in(jax.random.fold_in(own_key, 6), axis_at), (blocks,), jnp.float32, low / len(cuts), top_value / len(cuts))
        gain = gain * jnp.repeat(jnp.exp(steps), dims[axis_at] // blocks).reshape((-1,) + (1,) * (len(dims) - 1 - axis_at))
    return gain


def noise(rng, shape, width, reach, pieces=(), dtype=jnp.bfloat16):
    array = jax.random.normal(rng, shape, jnp.float32) * width
    if len(pieces) > 0:
        array = block_scale(rng, shape, pieces, -0.22, 0.18) * array
    return jnp.clip(array, min=-reach, max=reach).astype(dtype)


def setup_inputs(seed: int = 0) -> dict:
    keys = jax.random.split(jax.random.key(seed), 5)
    return {
        "field": noise(keys[0], (N, N, N), 1.0, 6.0, ((0, 8), (1, 4)), jnp.float32),
        "forward": noise(keys[1], (2, HALF, HALF), HALF ** -0.5, 0.375, (), jnp.float32),
        "inverse": noise(keys[2], (2, HALF, HALF), HALF ** -0.5, 0.375, (), jnp.float32),
        "eigen": jnp.clip(jnp.exp(jax.random.uniform(keys[3], (N,), jnp.float32, math.log(0.05), math.log(20.0))), 0.05, 20.0),
    }


def along_first(matrix, values):
    halves = matrix.shape[1]
    shape_in = values.shape
    blocks = values.reshape(2, halves, -1)
    result = jnp.einsum('pkm,pmr->pkr', matrix, blocks, precision=lax.Precision.HIGHEST)
    return result.reshape(shape_in)


def along_middle(matrix, values):
    halves = matrix.shape[1]
    shape_in = values.shape
    blocks = values.reshape(shape_in[0], 2, halves, shape_in[2])
    result = jnp.einsum('pkm,ipmy->ipky', matrix, blocks, precision=lax.Precision.HIGHEST)
    return result.reshape(shape_in)


def along_last(matrix, values):
    halves = matrix.shape[1]
    shape_in = values.shape
    blocks = values.reshape(-1, 2, halves)
    result = jnp.einsum('rpm,pkm->rpk', blocks, matrix, precision=lax.Precision.HIGHEST)
    return result.reshape(shape_in)


def reference(field, forward, inverse, eigen):
    spectral = along_last(forward, field)
    spectral = along_middle(forward, spectral)
    spectral = along_first(forward, spectral)
    denominator = eigen[:, None, None] + eigen[None, :, None] + eigen[None, None, :]
    spectral = spectral / denominator
    spectral = along_first(inverse, spectral)
    spectral = along_middle(inverse, spectral)
    return along_last(inverse, spectral)
```

```python
import math

import jax
import jax.numpy as jnp
from jax import lax
from jax.experimental import pallas as pl
from jax.experimental.pallas import tpu as pltpu
from jax.sharding import Mesh, PartitionSpec as P

AXES = ("xl", "gy", "zl")
LANES = 128
CHUNKS = ((16, 0), (12, 12), (0, 16))


def split(x):
    high = x.astype(jnp.bfloat16)
    low = (x - high.astype(jnp.float32)).astype(jnp.bfloat16)
    return high, low


def dot3(a, b, dims):
    ah, al = a
    bh, bl = b
    dot = lambda u, v: lax.dot_general(u, v, (dims, ((), ())), preferred_element_type=jnp.float32)
    return dot(ah, bh) + (dot(ah, bl) + dot(al, bh))


def swap_blocks(x, index, axis):
    count = x.shape[axis]
    bits = count.bit_length() - 1
    shape = x.shape
    x = x.reshape(shape[:axis] + (2,) * bits + shape[axis + 1:])
    for bit in range(bits):
        at = axis + bits - 1 - bit
        x = jnp.where((index >> bit) & 1 == 1, jnp.flip(x, at), x)
    return x.reshape(shape)


def pad_last(x, axis, to):
    widths = [(0, 0)] * x.ndim
    widths[axis] = (0, to - x.shape[axis])
    return jnp.pad(x, widths)


def first_kernel(field_ref, weight_ref, *out_refs):
    width = weight_ref.shape[1]
    weight = split(weight_ref[...])
    values = split(field_ref[:, :width])
    result = dot3(weight, values, ((1,), (1,)))
    rows = out_refs[0].shape[0]
    for d, out in enumerate(out_refs):
        out[...] = result[d * rows:(d + 1) * rows]


def first_step(field, weight, count, block):
    cells, width = field.shape
    rows = weight.shape[0] // count
    in_width = min(width, weight.shape[1]) if weight.shape[1] % LANES == 0 else width
    return pl.pallas_call(
        first_kernel,
        grid=(cells // block,),
        in_specs=[
            pl.BlockSpec((block, in_width), lambda r: (r, 0)),
            pl.BlockSpec(weight.shape, lambda r: (0, 0)),
        ],
        out_specs=[pl.BlockSpec((rows, block), lambda r: (0, r))] * count,
        out_shape=[jax.ShapeDtypeStruct((rows, cells), jnp.float32)] * count,
        cost_estimate=pl.CostEstimate(flops=6 * cells * weight.size, bytes_accessed=4 * cells * (width + rows * count), transcendentals=0),
        name="first",
    )(field, weight)


def middle_kernel(i_local, k_local, count, eig_ref, ek_ref, ei_ref, fk_ref, fi_ref, gi_ref, gk_ref, *refs):
    ins, outs, work = refs[:count], refs[count:2 * count], refs[2 * count:]
    rows = ins[0].shape[0]
    i_blocks = count // 2
    period = math.lcm(k_local, LANES)
    i_per, tiles = period // k_local, period // LANES
    lane = lax.broadcasted_iota(jnp.int32, (rows, LANES), 1)

    for dy in range(i_blocks):
        def spread(g, _, dy=dy):
            base = pl.multiple_of(g * period, LANES)
            for half in range(2):
                ref = ins[2 * dy + half]
                data = [ref[:, pl.ds(base + LANES * q, LANES)] for q in range(tiles)]
                for t in range(i_per):
                    q, off = divmod(t * k_local, LANES)
                    x = data[q]
                    if off + k_local > LANES:
                        x = jnp.where(lane >= off, x, data[q + 1])
                    if off:
                        x = pltpu.roll(x, LANES - off, 1)
                    at = pl.multiple_of((dy * i_local + g * i_per + t) * rows, 8)
                    work[half][pl.ds(at, rows), :] = x
            return 0
        lax.fori_loop(0, i_local // i_per, spread, 0)

    fk, fi, gi, gk = split(fk_ref[...]), split(fi_ref[...]), split(gi_ref[...]), split(gk_ref[...])
    size = i_blocks * i_local
    eigen_ik = ei_ref[...] + ek_ref[...]

    def solve(j, _):
        x = jnp.concatenate([ref[pl.ds(j, size, stride=rows), :] for ref in work], axis=1)
        x = dot3(split(x), fk, ((1,), (0,)))
        x = dot3(fi, split(x), ((1,), (0,)))
        x = x / (eigen_ik + eig_ref[0, j])
        x = dot3(gi, split(x), ((1,), (0,)))
        x = dot3(split(x), gk, ((1,), (0,)))
        for half, ref in enumerate(work):
            ref[pl.ds(j, size, stride=rows), :] = x[:, half * LANES:(half + 1) * LANES]
        return 0
    lax.fori_loop(0, rows, solve, 0)

    for dy in range(i_blocks):
        def gather(g, _, dy=dy):
            base = pl.multiple_of(g * period, LANES)
            for half in range(2):
                data = []
                for t in range(i_per):
                    at = pl.multiple_of((dy * i_local + g * i_per + t) * rows, 8)
                    data.append(work[half][pl.ds(at, rows), :])
                for q in range(tiles):
                    t, off = divmod(q * LANES, k_local)
                    left = k_local - off
                    x = pltpu.roll(data[t], LANES - off, 1) if off else data[t]
                    if left < LANES:
                        x = jnp.where(lane < left, x, pltpu.roll(data[t + 1], left, 1))
                    outs[2 * dy + half][:, pl.ds(base + LANES * q, LANES)] = x
            return 0
        lax.fori_loop(0, i_local // i_per, gather, 0)


def middle_step(pieces, eig, ek, ei, fk, fi, gi, gk, i_local, k_local):
    count = len(pieces)
    rows, cells = pieces[0].shape
    size = count // 2 * i_local
    vmem = pl.BlockSpec(memory_space=pltpu.VMEM)
    return pl.pallas_call(
        lambda *refs: middle_kernel(i_local, k_local, count, *refs),
        in_specs=[pl.BlockSpec(memory_space=pltpu.SMEM)] + [vmem] * (6 + count),
        out_specs=[vmem] * count,
        out_shape=[jax.ShapeDtypeStruct((rows, cells), jnp.float32)] * count,
        scratch_shapes=[pltpu.VMEM((size * rows, LANES), jnp.float32)] * 2,
        cost_estimate=pl.CostEstimate(flops=4 * 6 * rows * size * 256 * 256, bytes_accessed=8 * rows * cells * count, transcendentals=0),
        name="middle",
    )(eig, ek, ei, fk, fi, gi, gk, *pieces)


def last_kernel(counts, *refs):
    out_ref = refs[-1]
    total = None
    at = 0
    for count in counts:
        weight = split(refs[at][...])
        values = split(jnp.concatenate([ref[...] for ref in refs[at + 1:at + 1 + count]], axis=0))
        at += 1 + count
        part = dot3(values, weight, ((0,), (0,)))
        total = part if total is None else total + part
    out_ref[...] = total


def last_step(chunks, weights, block):
    cells = chunks[0][0].shape[1]
    width = weights[0].shape[1]
    operands, specs, flops = [], [], 0
    for pieces, weight in zip(chunks, weights):
        operands += [weight, *pieces]
        specs += [pl.BlockSpec(weight.shape, lambda r: (0, 0))]
        specs += [pl.BlockSpec((p.shape[0], block), lambda r: (0, r)) for p in pieces]
        flops += 6 * cells * weight.size
    return pl.pallas_call(
        lambda *refs: last_kernel([len(c) for c in chunks], *refs),
        grid=(cells // block,),
        in_specs=specs,
        out_specs=pl.BlockSpec((block, width), lambda r: (r, 0)),
        out_shape=jax.ShapeDtypeStruct((cells, width), jnp.float32),
        cost_estimate=pl.CostEstimate(flops=flops, bytes_accessed=8 * cells * width, transcendentals=0),
        name="last",
    )(*operands)


def block_rows(matrix, lead, sizes, starts, count, me):
    half = matrix.shape[1]
    parts = []
    for p in range(2):
        if sizes[p]:
            rows = matrix[p, starts[p]:starts[p] + count * sizes[p]].reshape(count, sizes[p], half)
            rows = swap_blocks(rows, me, 0)
            parts.append(jnp.pad(rows, ((0, 0), (0, 0), (p * half, (1 - p) * half))))
    rows = jnp.concatenate(parts, axis=1) if len(parts) > 1 else parts[0]
    rows = rows.reshape(-1, 2 * half)
    return rows[:, :lead]


def fast_body(count, field, forward, inverse, eigen):
    half = forward.shape[1]
    i_local, k_local, width = field.shape
    cells = i_local * k_local
    i_blocks = count // 2
    px, pz = lax.axis_index("px"), lax.axis_index("pz")
    me = lax.axis_index(AXES)
    me_l, me_i = me % 2, me // 2
    flat = field.reshape(cells, width)
    block = math.lcm(k_local, LANES)

    starts, at = [], (0, 0)
    for sizes in CHUNKS:
        starts.append(at)
        at = (at[0] + count * sizes[0], at[1] + count * sizes[1])

    def exchange(pieces):
        out = [pieces[0]]
        for d in range(1, count):
            out.append(lax.ppermute(pieces[d], AXES, [(s, s ^ d) for s in range(count)]))
        return out

    eigen2 = eigen.reshape(2, half)
    inverse_t = inverse.transpose(0, 2, 1)
    fk = swap_blocks(forward[pz].T.reshape(2, k_local, half), me_l, 0)
    fk = pad_last(fk, 1, LANES).reshape(2 * LANES, 2, k_local)
    fk = pad_last(fk, 2, LANES).reshape(2 * LANES, 2 * LANES)
    gk = swap_blocks(inverse_t[pz].reshape(half, 2, k_local), me_l, 1)
    gk = pad_last(gk, 2, LANES).reshape(2, k_local, 2 * LANES)
    gk = pad_last(gk, 1, LANES).reshape(2 * LANES, 2 * LANES)
    fi = swap_blocks(forward[px].reshape(half, i_blocks, i_local), me_i, 1).reshape(half, half)
    gi = swap_blocks(inverse[px].reshape(i_blocks, i_local, half), me_i, 0).reshape(half, half)
    ek = jnp.pad(eigen2[pz].reshape(2, k_local), ((0, 0), (0, LANES - k_local)), constant_values=1.0).reshape(1, 2 * LANES)
    ei = eigen2[px].reshape(half, 1)

    sent = []
    for sizes, start in zip(CHUNKS, starts):
        lead = -(-half // LANES) * LANES if sizes[1] == 0 else width
        weight = block_rows(forward, lead, sizes, start, count, me)
        sent.append(exchange(first_step(flat, weight, count, block)))
    back = []
    for sizes, start, pieces in zip(CHUNKS, starts, sent):
        eig = jnp.concatenate([lax.dynamic_slice_in_dim(eigen2[p], start[p] + me * sizes[p], sizes[p]) for p in range(2) if sizes[p]])
        done = middle_step(pieces, eig.reshape(1, -1), ek, ei, fk, fi, gi, gk, i_local, k_local)
        back.append(exchange(done))
    weights = [block_rows(inverse_t, width, sizes, start, count, me) for sizes, start in zip(CHUNKS, starts)]
    return last_step(back, weights, block).reshape(field.shape)


def plain_body(count_i, count_k, field, forward, inverse, eigen):
    half = forward.shape[1]
    i_local, k_local, width = field.shape
    count = count_i * count_k
    rows = width // count
    high = lax.Precision.HIGHEST
    px, pz = lax.axis_index("px"), lax.axis_index("pz")
    me = lax.axis_index(AXES)
    eigen2 = eigen.reshape(2, half)
    x = jnp.einsum("pjm,ikpm->pjik", forward, field.reshape(i_local, k_local, 2, half), precision=high)
    x = lax.all_to_all(x.reshape(count, rows, i_local, k_local), AXES, split_axis=0, concat_axis=0, tiled=True)
    x = x.reshape(count_i, count_k, rows, i_local, k_local).transpose(2, 0, 3, 1, 4).reshape(rows, half, half)
    x = jnp.einsum("nk,jik->jin", forward[pz], x, precision=high)
    x = jnp.einsum("ni,jik->jnk", forward[px], x, precision=high)
    eig = lax.dynamic_slice_in_dim(eigen, me * rows, rows)
    x = x / (eigen2[px][None, :, None] + eigen2[pz][None, None, :] + eig[:, None, None])
    x = jnp.einsum("ni,jik->jnk", inverse[px], x, precision=high)
    x = jnp.einsum("nk,jik->jin", inverse[pz], x, precision=high)
    x = x.reshape(rows, count_i, i_local, count_k, k_local).transpose(1, 3, 0, 2, 4).reshape(count, rows, i_local, k_local)
    x = lax.all_to_all(x, AXES, split_axis=0, concat_axis=0, tiled=True)
    x = jnp.einsum("pjm,pmik->ikpj", inverse, x.reshape(2, half, i_local, k_local), precision=high)
    return x.reshape(field.shape)


def solution(mesh):
    gx, gy, gz = (mesh.shape[name] for name in ("gx", "gy", "gz"))
    parts = Mesh(mesh.devices.reshape(2, gx // 2, gy, 2, gz // 2), ("px", "xl", "gy", "pz", "zl"))
    count_i, count_k = gx // 2 * gy, gz // 2

    def body(field, forward, inverse, eigen):
        i_local, k_local, width = field.shape
        fast = (
            count_k == 2
            and count_i & (count_i - 1) == 0
            and k_local <= LANES
            and width == count_i * count_k * sum(map(sum, CHUNKS))
            and i_local * k_local % math.lcm(k_local, LANES) == 0
        )
        if fast:
            return fast_body(count_i * count_k, field, forward, inverse, eigen)
        return plain_body(count_i, count_k, field, forward, inverse, eigen)

    spec = P(("px", "xl", "gy"), ("pz", "zl"), None)
    return jax.shard_map(body, mesh=parts, in_specs=(spec, P(), P(), P()), out_specs=spec, check_vma=False)
```

```python
import math

import jax
import jax.numpy as jnp
from jax import lax
from jax.experimental import pallas as pl
from jax.experimental.pallas import tpu as pltpu
from jax.sharding import Mesh, PartitionSpec as P

AXES = ("xl", "gy", "zl")
LANES = 128
CHUNKS = ((16, 0), (24, None), (16, 1))


def split(x):
    high = x.astype(jnp.bfloat16)
    low = (x - high.astype(jnp.float32)).astype(jnp.bfloat16)
    return high, low


def dot3(a, b, dims):
    ah, al = a
    bh, bl = b
    dot = lambda u, v: lax.dot_general(u, v, (dims, ((), ())), preferred_element_type=jnp.float32)
    return dot(ah, bh) + (dot(ah, bl) + dot(al, bh))


def halving(total):
    sizes = []
    while total:
        sizes.append(-(-total // 2))
        total -= sizes[-1]
    return sizes


def sending_order(count):
    far = [d for d in range(2, count) if 2 * d >= count]
    near = [d for d in range(1, count) if d not in far]
    order = [0]
    for pair in zip([d for d in far if d % 2 == 0], [d for d in near if d % 2 == 1]):
        order += pair
    return order + [d for d in far + near if d not in order]


def shares(count, chunk):
    return [count // 2 if chunk[1] is None else count * (chunk[1] == p) for p in range(2)]


def swap_blocks(x, index, axis):
    count = x.shape[axis]
    bits = count.bit_length() - 1
    shape = x.shape
    x = x.reshape(shape[:axis] + (2,) * bits + shape[axis + 1:])
    for bit in range(bits):
        at = axis + bits - 1 - bit
        x = jnp.where((index >> bit) & 1 == 1, jnp.flip(x, at), x)
    return x.reshape(shape)


def pad_last(x, axis, to):
    widths = [(0, 0)] * x.ndim
    widths[axis] = (0, to - x.shape[axis])
    return jnp.pad(x, widths)


def load_field(field_ref, data, sems, start, block):
    step = pl.program_id(0)
    copies = data.shape[0] // block

    def copy(r):
        source = field_ref.at[pl.ds((start + r) * block, block), pl.ds(0, data.shape[1])]
        return pltpu.make_async_copy(source, data.at[pl.ds(r * block, block), :], sems.at[r])

    @pl.when(step == 0)
    def _():
        for r in range(copies):
            copy(r).start()

    copy(step).wait()
    return data[pl.ds(pl.multiple_of(step * block, 8), block), :]


def write_pieces(result, out_refs):
    rows = out_refs[0].shape[0]
    for d, out in zip(sending_order(len(out_refs)), out_refs):
        out[...] = result[d * rows:(d + 1) * rows]


def lead_kernel(count, start, block, me_ref, forward_ref, field_ref, _, *refs):
    outs, (data, sems, matrix, weight_sem) = refs[:count], refs[count:]
    half = forward_ref.shape[2]
    rows = outs[0].shape[0]
    get = pltpu.make_async_copy(forward_ref.at[0], matrix, weight_sem)

    @pl.when(pl.program_id(0) == 0)
    def _():
        get.start()

    values = load_field(field_ref, data, sems, start, block)[:, :half]

    @pl.when(pl.program_id(0) == 0)
    def _():
        get.wait()

    weight = jnp.concatenate([matrix[pl.ds(pl.multiple_of((me_ref[0] ^ d) * rows, 8), rows), :] for d in range(count)], axis=0)
    write_pieces(dot3(split(weight), split(values), ((1,), (1,))), outs)


def next_kernel(count, start, block, weight_ref, field_ref, _, *refs):
    outs, (data, sems) = refs[:count], refs[count:]
    values = load_field(field_ref, data, sems, start, block)
    write_pieces(dot3(split(weight_ref[...]), split(values), ((1,), (1,))), outs)


def first_step(kernel, operands, specs, scratch, field, after, rows, count, start, number, width, block, name):
    hbm = pl.BlockSpec(memory_space=pl.ANY)
    return pl.pallas_call(
        lambda *refs: kernel(count, start, block, *refs),
        grid=(number,),
        in_specs=[*specs, hbm, hbm],
        out_specs=[pl.BlockSpec((rows, block), lambda r: (0, r))] * count,
        out_shape=[jax.ShapeDtypeStruct((rows, number * block), jnp.float32)] * count,
        scratch_shapes=[pltpu.VMEM((number * block, width), jnp.float32), pltpu.SemaphoreType.DMA((number,)), *scratch],
        cost_estimate=pl.CostEstimate(flops=6 * number * block * width * rows * count, bytes_accessed=4 * number * block * (width + rows * count), transcendentals=0),
        name=name,
    )(*operands, field, after)


def middle_kernel(i_local, k_local, count, units_in, units, eig_ref, ek_ref, ei_ref, fk_ref, fi_ref, gi_ref, gk_ref, *refs):
    given = count * len(units_in)
    ins, outs, work = refs[:given], refs[given:-2], refs[-2:]
    rows = ins[0].shape[0]
    place = [sending_order(count).index(d) for d in range(count)]
    i_blocks = count // 2
    period = math.lcm(k_local, LANES)
    i_per, tiles = period // k_local, period // LANES
    lane = lax.broadcasted_iota(jnp.int32, (rows, LANES), 1)

    for dy in range(i_blocks):
        begin = 0
        for s, number in enumerate(units_in):
            def spread(g, _, dy=dy, s=s, begin=begin):
                base = pl.multiple_of(g * period, LANES)
                for half in range(2):
                    ref = ins[s * count + place[2 * dy + half]]
                    data = [ref[:, pl.ds(base + LANES * q, LANES)] for q in range(tiles)]
                    for t in range(i_per):
                        q, off = divmod(t * k_local, LANES)
                        x = data[q]
                        if off + k_local > LANES:
                            x = jnp.where(lane >= off, x, data[q + 1])
                        if off:
                            x = pltpu.roll(x, LANES - off, 1)
                        at = pl.multiple_of((dy * i_local + (begin + g) * i_per + t) * rows, 8)
                        work[half][pl.ds(at, rows), :] = x
                return 0
            lax.fori_loop(0, number, spread, 0)
            begin += number

    fk, fi, gi, gk = split(fk_ref[...]), split(fi_ref[...]), split(gi_ref[...]), split(gk_ref[...])
    size = i_blocks * i_local
    eigen_ik = ei_ref[...] + ek_ref[...]

    def solve(j, _):
        x = jnp.concatenate([ref[pl.ds(j, size, stride=rows), :] for ref in work], axis=1)
        x = dot3(split(x), fk, ((1,), (0,)))
        x = dot3(fi, split(x), ((1,), (0,)))
        x = x / (eigen_ik + eig_ref[0, j])
        x = dot3(gi, split(x), ((1,), (0,)))
        x = dot3(split(x), gk, ((1,), (0,)))
        for half, ref in enumerate(work):
            ref[pl.ds(j, size, stride=rows), :] = x[:, half * LANES:(half + 1) * LANES]
        return 0
    lax.fori_loop(0, rows, solve, 0)

    for dy in range(i_blocks):
        begin = 0
        for s, number in enumerate(units):
            def gather(g, _, dy=dy, s=s, begin=begin):
                base = pl.multiple_of(g * period, LANES)
                for half in range(2):
                    data = []
                    for t in range(i_per):
                        at = pl.multiple_of((dy * i_local + (begin + g) * i_per + t) * rows, 8)
                        data.append(work[half][pl.ds(at, rows), :])
                    for q in range(tiles):
                        t, off = divmod(q * LANES, k_local)
                        left = k_local - off
                        x = pltpu.roll(data[t], LANES - off, 1) if off else data[t]
                        if left < LANES:
                            x = jnp.where(lane < left, x, pltpu.roll(data[t + 1], left, 1))
                        outs[s * count + place[2 * dy + half]][:, pl.ds(base + LANES * q, LANES)] = x
                return 0
            lax.fori_loop(0, number, gather, 0)
            begin += number


def middle_step(sent, eig, ek, ei, fk, fi, gi, gk, i_local, k_local, units_in, units):
    count = len(sent[0])
    rows = sent[0][0].shape[0]
    cells = i_local * k_local
    size = count // 2 * i_local
    vmem = pl.BlockSpec(memory_space=pltpu.VMEM)
    unit = cells // sum(units)
    pieces = [piece for part in sent for piece in part]
    outs = pl.pallas_call(
        lambda *refs: middle_kernel(i_local, k_local, count, units_in, units, *refs),
        in_specs=[pl.BlockSpec(memory_space=pltpu.SMEM)] + [vmem] * (6 + len(pieces)),
        out_specs=[vmem] * (count * len(units)),
        out_shape=[jax.ShapeDtypeStruct((rows, n * unit), jnp.float32) for n in units for _ in range(count)],
        scratch_shapes=[pltpu.VMEM((size * rows, LANES), jnp.float32)] * 2,
        cost_estimate=pl.CostEstimate(flops=4 * 6 * rows * size * 256 * 256, bytes_accessed=8 * rows * cells * count, transcendentals=0),
        name="middle",
    )(eig, ek, ei, fk, fi, gi, gk, *pieces)
    return [outs[s * count:(s + 1) * count] for s in range(len(units))]


def last_kernel(count, start, blocks, upper_ref, weight_ref, *refs):
    total = count * len(CHUNKS)
    pieces = refs[:total]
    out_ref, stage, result, matrix, in_sems, out_sems = refs[-6:]
    half = weight_ref.shape[2]
    get = pltpu.make_async_copy(weight_ref, matrix, out_sems.at[len(blocks)])
    get.start()

    def copies(b, at, size):
        found, row = [], 0
        for n, piece in enumerate(pieces):
            rows = piece.shape[0]
            base = start if n < total - count else 0
            to = row + sending_order(count)[n % count] * rows
            found.append(pltpu.make_async_copy(piece.at[:, pl.ds(base + at, size)], stage.at[pl.ds(to, rows), pl.ds(at, size)], in_sems.at[b, n]))
            if n % count == count - 1:
                row += count * rows
        return found

    def put(b, at, size):
        return pltpu.make_async_copy(result.at[pl.ds(at, size), :], out_ref.at[pl.ds(start + at, size), :], out_sems.at[b])

    spans = [(b, sum(blocks[:b]), size) for b, size in enumerate(blocks)]
    for span in spans:
        for copy in copies(*span):
            copy.start()
    get.wait()
    weights = [split(matrix[p]) for p in range(2)]
    for b, at, size in spans:
        for copy in copies(b, at, size):
            copy.wait()
        for p in range(2):
            parts, row = [], 0
            for chunk in CHUNKS:
                rows = shares(count, chunk)[p] * chunk[0]
                if chunk[1] is None:
                    parts.append(stage[pl.ds(pl.multiple_of(row + (upper_ref[0] ^ p) * rows, 8), rows), at:at + size])
                elif rows:
                    parts.append(stage[row:row + rows, at:at + size])
                row += count * chunk[0]
            values = split(jnp.concatenate(parts, axis=0))
            result[at:at + size, p * half:(p + 1) * half] = dot3(values, weights[p], ((0,), (0,)))
        put(b, at, size).start()
    for span in spans:
        put(*span).wait()


def last_step(upper, weight, chunks, out, start, blocks, cells, width):
    pieces = [piece for chunk in chunks for piece in chunk]
    operands = [upper, weight, *pieces]
    hbm = pl.BlockSpec(memory_space=pl.ANY)
    specs = [pl.BlockSpec(memory_space=pltpu.SMEM)] + [hbm] * (1 + len(pieces))
    aliases = {}
    if out is not None:
        aliases = {len(operands): 0}
        operands.append(out)
        specs.append(hbm)
    lanes = sum(blocks)
    return pl.pallas_call(
        lambda *refs: last_kernel(len(chunks[0]), start, blocks, *refs),
        in_specs=specs,
        out_specs=hbm,
        out_shape=jax.ShapeDtypeStruct((cells, width), jnp.float32),
        input_output_aliases=aliases,
        scratch_shapes=[
            pltpu.VMEM((sum(piece.shape[0] for piece in pieces), lanes), jnp.float32),
            pltpu.VMEM((lanes, width), jnp.float32),
            pltpu.VMEM(weight.shape, jnp.float32),
            pltpu.SemaphoreType.DMA((len(blocks), len(pieces))),
            pltpu.SemaphoreType.DMA((len(blocks) + 1,)),
        ],
        cost_estimate=pl.CostEstimate(flops=6 * lanes * weight.size, bytes_accessed=8 * lanes * width, transcendentals=0),
        name="last",
    )(*operands)


def block_rows(matrix, chunk, starts, count, me):
    half = matrix.shape[1]
    parts = []
    for p, share in enumerate(shares(count, chunk)):
        if share:
            rows = matrix[p, starts[p]:starts[p] + share * chunk[0]]
            parts.append(jnp.pad(rows, ((0, 0), (p * half, (1 - p) * half))))
    rows = jnp.concatenate(parts, axis=0).reshape(count, chunk[0], 2 * half)
    return swap_blocks(rows, me, 0).reshape(-1, 2 * half)


def parity_rows(matrix, starts, count, me):
    sides = []
    for p in range(2):
        parts = []
        for chunk, start in zip(CHUNKS, starts):
            share = shares(count, chunk)[p]
            if share:
                rows = matrix[p, start[p]:start[p] + share * chunk[0]].reshape(share, chunk[0], -1)
                parts.append(swap_blocks(rows, me % share, 0).reshape(share * chunk[0], -1))
        sides.append(jnp.concatenate(parts, axis=0))
    return jnp.stack(sides)


def fast_body(count, field, forward, inverse, eigen):
    half = forward.shape[1]
    i_local, k_local, width = field.shape
    cells = i_local * k_local
    i_blocks = count // 2
    px, pz = lax.axis_index("px"), lax.axis_index("pz")
    me = lax.axis_index(AXES)
    me_l, me_i, upper = me % 2, me // 2, me // (count // 2)
    flat = field.reshape(cells, width)
    block = math.lcm(k_local, LANES)
    total = cells // block

    starts, at = [], (0, 0)
    for chunk in CHUNKS:
        starts.append(at)
        at = tuple(a + n * chunk[0] for a, n in zip(at, shares(count, chunk)))

    order = sending_order(count)

    def exchange(pieces):
        return [pieces[0]] + [lax.ppermute(piece, AXES, [(s, s ^ d) for s in range(count)]) for d, piece in zip(order[1:], pieces[1:])]

    vmem, smem, hbm = (pl.BlockSpec(memory_space=space) for space in (pltpu.VMEM, pltpu.SMEM, pl.ANY))
    scratch = [pltpu.VMEM((half, half), jnp.float32), pltpu.SemaphoreType.DMA]
    lead_width = -(-half // LANES) * LANES
    cut_in = [[total // 2, total - total // 2]] + [[total]] * (len(CHUNKS) - 1)
    cut_out = [[total]] * (len(CHUNKS) - 1) + [halving(total)]
    sent = [[]]
    after, start = flat, 0
    for number in cut_in[0]:
        pieces = first_step(lead_kernel, (me.reshape(1), forward), [smem, hbm], scratch, flat, after, CHUNKS[0][0], count, start, number, lead_width, block, "lead")
        sent[0].append(exchange(pieces))
        after = pieces[0]
        start += number
    forward, inverse, eigen, _ = lax.optimization_barrier((forward, inverse, eigen, after))
    for chunk, start in zip(CHUNKS[1:], starts[1:]):
        weight = block_rows(forward, chunk, start, count, me)
        pieces = first_step(next_kernel, (weight,), [vmem], [], flat, after, chunk[0], count, 0, total, width, block, "next")
        sent.append([exchange(pieces)])
        after = pieces[0]

    eigen2 = eigen.reshape(2, half)
    inverse_t = inverse.transpose(0, 2, 1)
    fk = swap_blocks(forward[pz].T.reshape(2, k_local, half), me_l, 0)
    fk = pad_last(fk, 1, LANES).reshape(2 * LANES, 2, k_local)
    fk = pad_last(fk, 2, LANES).reshape(2 * LANES, 2 * LANES)
    gk = swap_blocks(inverse_t[pz].reshape(half, 2, k_local), me_l, 1)
    gk = pad_last(gk, 2, LANES).reshape(2, k_local, 2 * LANES)
    gk = pad_last(gk, 1, LANES).reshape(2 * LANES, 2 * LANES)
    fi = swap_blocks(forward[px].reshape(half, i_blocks, i_local), me_i, 1).reshape(half, half)
    gi = swap_blocks(inverse[px].reshape(i_blocks, i_local, half), me_i, 0).reshape(half, half)
    ek = jnp.pad(eigen2[pz].reshape(2, k_local), ((0, 0), (0, LANES - k_local)), constant_values=1.0).reshape(1, 2 * LANES)
    ei = eigen2[px].reshape(half, 1)

    back = []
    for chunk, start, parts, units_in, units in zip(CHUNKS, starts, sent, cut_in, cut_out):
        if chunk[1] is None:
            own = upper * half + jnp.where(upper == 1, start[1], start[0]) + me % (count // 2) * chunk[0]
        else:
            own = chunk[1] * half + start[chunk[1]] + me * chunk[0]
        eig = lax.dynamic_slice_in_dim(eigen, own, chunk[0]).reshape(1, -1)
        done = middle_step(parts, eig, ek, ei, fk, fi, gi, gk, i_local, k_local, units_in, units)
        back.append([exchange(part) for part in done])
    weight = parity_rows(inverse_t, starts, count, me)
    whole = [parts[0] for parts in back[:-1]]
    out, at = None, 0
    for tail, number in zip(back[-1], cut_out[-1]):
        final = at + number * block == cells
        blocks = [LANES * n for n in halving(block // LANES)[:1]] if final else [block] * number
        if final:
            blocks.append(block - blocks[0])
        out = last_step(upper.reshape(1), weight, [*whole, tail], out, at, blocks, cells, width)
        at += number * block
    return out.reshape(field.shape)


def plain_body(count_i, count_k, field, forward, inverse, eigen):
    half = forward.shape[1]
    i_local, k_local, width = field.shape
    count = count_i * count_k
    rows = width // count
    high = lax.Precision.HIGHEST
    px, pz = lax.axis_index("px"), lax.axis_index("pz")
    me = lax.axis_index(AXES)
    eigen2 = eigen.reshape(2, half)
    x = jnp.einsum("pjm,ikpm->pjik", forward, field.reshape(i_local, k_local, 2, half), precision=high)
    x = lax.all_to_all(x.reshape(count, rows, i_local, k_local), AXES, split_axis=0, concat_axis=0, tiled=True)
    x = x.reshape(count_i, count_k, rows, i_local, k_local).transpose(2, 0, 3, 1, 4).reshape(rows, half, half)
    x = jnp.einsum("nk,jik->jin", forward[pz], x, precision=high)
    x = jnp.einsum("ni,jik->jnk", forward[px], x, precision=high)
    eig = lax.dynamic_slice_in_dim(eigen, me * rows, rows)
    x = x / (eigen2[px][None, :, None] + eigen2[pz][None, None, :] + eig[:, None, None])
    x = jnp.einsum("ni,jik->jnk", inverse[px], x, precision=high)
    x = jnp.einsum("nk,jik->jin", inverse[pz], x, precision=high)
    x = x.reshape(rows, count_i, i_local, count_k, k_local).transpose(1, 3, 0, 2, 4).reshape(count, rows, i_local, k_local)
    x = lax.all_to_all(x, AXES, split_axis=0, concat_axis=0, tiled=True)
    x = jnp.einsum("pjm,pmik->ikpj", inverse, x.reshape(2, half, i_local, k_local), precision=high)
    return x.reshape(field.shape)


def solution(mesh):
    gx, gy, gz = (mesh.shape[name] for name in ("gx", "gy", "gz"))
    parts = Mesh(mesh.devices.reshape(2, gx // 2, gy, 2, gz // 2), ("px", "xl", "gy", "pz", "zl"))
    count_i, count_k = gx // 2 * gy, gz // 2

    def body(field, forward, inverse, eigen):
        i_local, k_local, width = field.shape
        fast = (
            count_k == 2
            and count_i & (count_i - 1) == 0
            and k_local <= LANES
            and width == count_i * count_k * sum(chunk[0] for chunk in CHUNKS)
            and i_local * k_local % math.lcm(k_local, LANES) == 0
            and i_local * k_local > math.lcm(k_local, LANES)
        )
        if fast:
            return fast_body(count_i * count_k, field, forward, inverse, eigen)
        return plain_body(count_i, count_k, field, forward, inverse, eigen)

    spec = P(("px", "xl", "gy"), ("pz", "zl"), None)
    return jax.shard_map(body, mesh=parts, in_specs=(spec, P(), P(), P()), out_specs=spec, check_vma=False)
```

```python
import math

import jax
import jax.numpy as jnp
from jax import lax
from jax.experimental import pallas as pl
from jax.experimental.pallas import tpu as pltpu
from jax.sharding import Mesh, PartitionSpec as P


AXES = ("xl", "gy", "zl")
LANES = 128
CHUNKS = ((16, 0), (24, None), (16, 1))


def split(x):
    high = x.astype(jnp.bfloat16)
    low = (x - high.astype(jnp.float32)).astype(jnp.bfloat16)
    return high, low


def dot3(a, b, dims):
    ah, al = a
    bh, bl = b
    dot = lambda u, v: lax.dot_general(u, v, (dims, ((), ())), preferred_element_type=jnp.float32)
    return dot(ah, bh) + (dot(ah, bl) + dot(al, bh))


def cut(total, parts):
    sizes = []
    for left in range(parts, 0, -1):
        sizes.append(-(-(total - sum(sizes)) // left))
    return sizes


def sending_order(count):
    far = [d for d in range(2, count) if 2 * d >= count]
    near = [d for d in range(1, count) if d not in far]
    order = [0]
    for pair in zip([d for d in far if d % 2 == 0], [d for d in near if d % 2 == 1]):
        order += pair
    return order + [d for d in far + near if d not in order]


def shares(count, chunk):
    return [count // 2 if chunk[1] is None else count * (chunk[1] == p) for p in range(2)]


def swap_blocks(x, index, axis):
    count = x.shape[axis]
    bits = count.bit_length() - 1
    shape = x.shape
    x = x.reshape(shape[:axis] + (2,) * bits + shape[axis + 1:])
    for bit in range(bits):
        at = axis + bits - 1 - bit
        x = jnp.where((index >> bit) & 1 == 1, jnp.flip(x, at), x)
    return x.reshape(shape)


def pad_last(x, axis, to):
    widths = [(0, 0)] * x.ndim
    widths[axis] = (0, to - x.shape[axis])
    return jnp.pad(x, widths)


def load_field(field_ref, data, sems, start, block):
    step = pl.program_id(0)
    copies = data.shape[0] // block

    def copy(r):
        source = field_ref.at[pl.ds((start + r) * block, block), pl.ds(0, data.shape[1])]
        return pltpu.make_async_copy(source, data.at[pl.ds(r * block, block), :], sems.at[r])

    @pl.when(step == 0)
    def _():
        for r in range(copies):
            copy(r).start()

    copy(step).wait()
    return data[pl.ds(pl.multiple_of(step * block, 8), block), :]


def write_pieces(result, out_refs):
    rows = out_refs[0].shape[0]
    for d, out in zip(sending_order(len(out_refs)), out_refs):
        out[...] = result[d * rows:(d + 1) * rows]


def lead_kernel(count, start, block, me_ref, forward_ref, field_ref, _, *refs):
    outs, (data, sems, matrix, weight_sem) = refs[:count], refs[count:]
    half = forward_ref.shape[2]
    rows = outs[0].shape[0]
    get = pltpu.make_async_copy(forward_ref.at[0], matrix, weight_sem)

    @pl.when(pl.program_id(0) == 0)
    def _():
        get.start()

    values = load_field(field_ref, data, sems, start, block)[:, :half]

    @pl.when(pl.program_id(0) == 0)
    def _():
        get.wait()

    weight = jnp.concatenate([matrix[pl.ds(pl.multiple_of((me_ref[0] ^ d) * rows, 8), rows), :] for d in range(count)], axis=0)
    write_pieces(dot3(split(weight), split(values), ((1,), (1,))), outs)


def next_kernel(count, start, block, weight_ref, field_ref, _, *refs):
    outs, (data, sems) = refs[:count], refs[count:]
    values = load_field(field_ref, data, sems, start, block)
    write_pieces(dot3(split(weight_ref[...]), split(values), ((1,), (1,))), outs)


def first_step(kernel, operands, specs, scratch, field, after, rows, count, start, number, width, block):
    hbm = pl.BlockSpec(memory_space=pl.ANY)
    return pl.pallas_call(
        lambda *refs: kernel(count, start, block, *refs),
        grid=(number,),
        in_specs=[*specs, hbm, hbm],
        out_specs=[pl.BlockSpec((rows, block), lambda r: (0, r))] * count,
        out_shape=[jax.ShapeDtypeStruct((rows, number * block), jnp.float32)] * count,
        scratch_shapes=[pltpu.VMEM((number * block, width), jnp.float32), pltpu.SemaphoreType.DMA((number,)), *scratch],
        cost_estimate=pl.CostEstimate(flops=6 * number * block * width * rows * count, bytes_accessed=4 * number * block * (width + rows * count), transcendentals=0),
    )(*operands, field, after)


def middle_kernel(i_local, k_local, count, units_in, units, eig_ref, ek_ref, ei_ref, fk_ref, fi_ref, gi_ref, gk_ref, *refs):
    given = count * len(units_in)
    ins, outs, work = refs[:given], refs[given:-2], refs[-2:]
    rows = ins[0].shape[0]
    place = [sending_order(count).index(d) for d in range(count)]
    i_blocks = count // 2
    period = math.lcm(k_local, LANES)
    i_per, tiles = period // k_local, period // LANES
    lane = lax.broadcasted_iota(jnp.int32, (rows, LANES), 1)

    for dy in range(i_blocks):
        begin = 0
        for s, number in enumerate(units_in):
            def spread(g, _, dy=dy, s=s, begin=begin):
                base = pl.multiple_of(g * period, LANES)
                for half in range(2):
                    ref = ins[s * count + place[2 * dy + half]]
                    data = [ref[:, pl.ds(base + LANES * q, LANES)] for q in range(tiles)]
                    for t in range(i_per):
                        q, off = divmod(t * k_local, LANES)
                        x = data[q]
                        if off + k_local > LANES:
                            x = jnp.where(lane >= off, x, data[q + 1])
                        if off:
                            x = pltpu.roll(x, LANES - off, 1)
                        at = pl.multiple_of((dy * i_local + (begin + g) * i_per + t) * rows, 8)
                        work[half][pl.ds(at, rows), :] = x
                return 0

            lax.fori_loop(0, number, spread, 0)
            begin += number

    fk, fi, gi, gk = split(fk_ref[...]), split(fi_ref[...]), split(gi_ref[...]), split(gk_ref[...])
    size = i_blocks * i_local
    eigen_ik = ei_ref[...] + ek_ref[...]

    def solve(j, _):
        x = jnp.concatenate([ref[pl.ds(j, size, stride=rows), :] for ref in work], axis=1)
        x = dot3(split(x), fk, ((1,), (0,)))
        x = dot3(fi, split(x), ((1,), (0,)))
        x = x / (eigen_ik + eig_ref[0, j])
        x = dot3(gi, split(x), ((1,), (0,)))
        x = dot3(split(x), gk, ((1,), (0,)))
        for half, ref in enumerate(work):
            ref[pl.ds(j, size, stride=rows), :] = x[:, half * LANES:(half + 1) * LANES]
        return 0

    lax.fori_loop(0, rows, solve, 0)

    for dy in range(i_blocks):
        begin = 0
        for s, number in enumerate(units):
            def gather(g, _, dy=dy, s=s, begin=begin):
                base = pl.multiple_of(g * period, LANES)
                for half in range(2):
                    data = []
                    for t in range(i_per):
                        at = pl.multiple_of((dy * i_local + (begin + g) * i_per + t) * rows, 8)
                        data.append(work[half][pl.ds(at, rows), :])
                    for q in range(tiles):
                        t, off = divmod(q * LANES, k_local)
                        left = k_local - off
                        x = pltpu.roll(data[t], LANES - off, 1) if off else data[t]
                        if left < LANES:
                            x = jnp.where(lane < left, x, pltpu.roll(data[t + 1], left, 1))
                        outs[s * count + place[2 * dy + half]][:, pl.ds(base + LANES * q, LANES)] = x
                return 0

            lax.fori_loop(0, number, gather, 0)
            begin += number


def middle_step(sent, eig, ek, ei, fk, fi, gi, gk, i_local, k_local, units_in, units):
    count = len(sent[0])
    rows = sent[0][0].shape[0]
    cells = i_local * k_local
    size = count // 2 * i_local
    vmem = pl.BlockSpec(memory_space=pltpu.VMEM)
    unit = cells // sum(units)
    pieces = [piece for part in sent for piece in part]
    outs = pl.pallas_call(
        lambda *refs: middle_kernel(i_local, k_local, count, units_in, units, *refs),
        in_specs=[pl.BlockSpec(memory_space=pltpu.SMEM)] + [vmem] * (6 + len(pieces)),
        out_specs=[vmem] * (count * len(units)),
        out_shape=[jax.ShapeDtypeStruct((rows, n * unit), jnp.float32) for n in units for _ in range(count)],
        scratch_shapes=[pltpu.VMEM((size * rows, LANES), jnp.float32)] * 2,
        cost_estimate=pl.CostEstimate(flops=4 * 6 * rows * size * 256 * 256, bytes_accessed=8 * rows * cells * count, transcendentals=0),
        name="middle",
    )(eig, ek, ei, fk, fi, gi, gk, *pieces)
    return [outs[s * count:(s + 1) * count] for s in range(len(units))]


def last_kernel(count, start, blocks, upper_ref, weight_ref, *refs):
    total = count * len(CHUNKS)
    pieces = refs[-6 - total:-6]
    out_ref, stage, result, matrix, in_sems, out_sems = refs[-6:]
    half = weight_ref.shape[2]
    get = pltpu.make_async_copy(weight_ref, matrix, out_sems.at[len(blocks)])
    get.start()

    def copies(b, at, size):
        found, row = [], 0
        for n, piece in enumerate(pieces):
            rows = piece.shape[0]
            base = start if n < total - count else 0
            to = row + sending_order(count)[n % count] * rows
            found.append(pltpu.make_async_copy(piece.at[:, pl.ds(base + at, size)], stage.at[pl.ds(to, rows), pl.ds(at, size)], in_sems.at[b, n]))
            if n % count == count - 1:
                row += count * rows
        return found

    def put(b, at, size):
        return pltpu.make_async_copy(result.at[pl.ds(at, size), :], out_ref.at[pl.ds(start + at, size), :], out_sems.at[b])

    spans = [(b, sum(blocks[:b]), size) for b, size in enumerate(blocks)]
    for span in spans:
        for copy in copies(*span):
            copy.start()
    get.wait()
    weights = [split(matrix[p]) for p in range(2)]
    for b, at, size in spans:
        for copy in copies(b, at, size):
            copy.wait()
        for p in range(2):
            parts, row = [], 0
            for chunk in CHUNKS:
                rows = shares(count, chunk)[p] * chunk[0]
                if chunk[1] is None:
                    parts.append(stage[pl.ds(pl.multiple_of(row + (upper_ref[0] ^ p) * rows, 8), rows), at:at + size])
                elif rows:
                    parts.append(stage[row:row + rows, at:at + size])
                row += count * chunk[0]
            values = split(jnp.concatenate(parts, axis=0))
            result[at:at + size, p * half:(p + 1) * half] = dot3(values, weights[p], ((0,), (0,)))
        put(b, at, size).start()
    for span in spans:
        put(*span).wait()


def last_step(upper, weight, chunks, out, start, blocks, cells, width):
    pieces = [piece for chunk in chunks for piece in chunk]
    before = [] if out is None else [out]
    operands = [upper, weight, *before, *pieces]
    hbm = pl.BlockSpec(memory_space=pl.ANY)
    specs = [pl.BlockSpec(memory_space=pltpu.SMEM)] + [hbm] * (len(operands) - 1)
    aliases = {2: 0} if before else {}
    lanes = sum(blocks)
    return pl.pallas_call(
        lambda *refs: last_kernel(len(chunks[0]), start, blocks, *refs),
        in_specs=specs,
        out_specs=hbm,
        out_shape=jax.ShapeDtypeStruct((cells, width), jnp.float32),
        input_output_aliases=aliases,
        scratch_shapes=[
            pltpu.VMEM((sum(piece.shape[0] for piece in pieces), lanes), jnp.float32),
            pltpu.VMEM((lanes, width), jnp.float32),
            pltpu.VMEM(weight.shape, jnp.float32),
            pltpu.SemaphoreType.DMA((len(blocks), len(pieces))),
            pltpu.SemaphoreType.DMA((len(blocks) + 1,)),
        ],
        cost_estimate=pl.CostEstimate(flops=6 * lanes * weight.size, bytes_accessed=8 * lanes * width, transcendentals=0),
        name="last",
    )(*operands)


def block_rows(matrix, chunk, starts, count, me):
    half = matrix.shape[1]
    parts = []
    for p, share in enumerate(shares(count, chunk)):
        if share:
            rows = matrix[p, starts[p]:starts[p] + share * chunk[0]]
            parts.append(jnp.pad(rows, ((0, 0), (p * half, (1 - p) * half))))
    rows = jnp.concatenate(parts, axis=0).reshape(count, chunk[0], 2 * half)
    return swap_blocks(rows, me, 0).reshape(-1, 2 * half)


def parity_rows(matrix, starts, count, me):
    sides = []
    for p in range(2):
        parts = []
        for chunk, start in zip(CHUNKS, starts):
            share = shares(count, chunk)[p]
            if share:
                rows = matrix[p, start[p]:start[p] + share * chunk[0]].reshape(share, chunk[0], -1)
                parts.append(swap_blocks(rows, me % share, 0).reshape(share * chunk[0], -1))
        sides.append(jnp.concatenate(parts, axis=0))
    return jnp.stack(sides)


def fast_body(count, field, forward, inverse, eigen):
    half = forward.shape[1]
    i_local, k_local, width = field.shape
    cells = i_local * k_local
    i_blocks = count // 2
    px, pz = lax.axis_index("px"), lax.axis_index("pz")
    me = lax.axis_index(AXES)
    me_l, me_i, upper = me % 2, me // 2, me // (count // 2)
    flat = field.reshape(cells, width)
    block = math.lcm(k_local, LANES)
    total = cells // block

    starts, at = [], (0, 0)
    for chunk in CHUNKS:
        starts.append(at)
        at = tuple(a + n * chunk[0] for a, n in zip(at, shares(count, chunk)))

    order = sending_order(count)

    def exchange(pieces):
        moved = [pieces[0]]
        for d, piece in zip(order[1:], pieces[1:]):
            moved.append(lax.ppermute(piece, AXES, [(s, s ^ d) for s in range(count)]))
        return moved

    vmem, smem, hbm = (pl.BlockSpec(memory_space=space) for space in (pltpu.VMEM, pltpu.SMEM, pl.ANY))
    scratch = [pltpu.VMEM((half, half), jnp.float32), pltpu.SemaphoreType.DMA]
    lead_width = -(-half // LANES) * LANES
    cut_in = [[total // 2, total - total // 2]] + [[total]] * (len(CHUNKS) - 1)
    cut_out = [[total]] * (len(CHUNKS) - 1) + [cut(total, min(total, 3))]
    sent = [[]]
    after, start = flat, 0
    for number in cut_in[0]:
        pieces = first_step(lead_kernel, (me.reshape(1), forward), [smem, hbm], scratch, flat, after, CHUNKS[0][0], count, start, number, lead_width, block)
        sent[0].append(exchange(pieces))
        after = pieces[0]
        start += number
    forward, inverse, eigen, _ = lax.optimization_barrier((forward, inverse, eigen, after))
    for chunk, start in zip(CHUNKS[1:], starts[1:]):
        weight = block_rows(forward, chunk, start, count, me)
        pieces = first_step(next_kernel, (weight,), [vmem], [], flat, after, chunk[0], count, 0, total, width, block)
        sent.append([exchange(pieces)])
        after = pieces[0]

    eigen2 = eigen.reshape(2, half)
    inverse_t = inverse.transpose(0, 2, 1)
    fk = swap_blocks(forward[pz].T.reshape(2, k_local, half), me_l, 0)
    fk = pad_last(fk, 1, LANES).reshape(2 * LANES, 2, k_local)
    fk = pad_last(fk, 2, LANES).reshape(2 * LANES, 2 * LANES)
    gk = swap_blocks(inverse_t[pz].reshape(half, 2, k_local), me_l, 1)
    gk = pad_last(gk, 2, LANES).reshape(2, k_local, 2 * LANES)
    gk = pad_last(gk, 1, LANES).reshape(2 * LANES, 2 * LANES)
    fi = swap_blocks(forward[px].reshape(half, i_blocks, i_local), me_i, 1).reshape(half, half)
    gi = swap_blocks(inverse[px].reshape(i_blocks, i_local, half), me_i, 0).reshape(half, half)
    ek = jnp.pad(eigen2[pz].reshape(2, k_local), ((0, 0), (0, LANES - k_local)), constant_values=1.0).reshape(1, 2 * LANES)
    ei = eigen2[px].reshape(half, 1)

    back = []
    for chunk, start, parts, units_in, units in zip(CHUNKS, starts, sent, cut_in, cut_out):
        if chunk[1] is None:
            own = upper * half + jnp.where(upper == 1, start[1], start[0]) + me % (count // 2) * chunk[0]
        else:
            own = chunk[1] * half + start[chunk[1]] + me * chunk[0]
        eig = lax.dynamic_slice_in_dim(eigen, own, chunk[0]).reshape(1, -1)
        done = middle_step(parts, eig, ek, ei, fk, fi, gi, gk, i_local, k_local, units_in, units)
        back.append([exchange(part) for part in done])
    weight = parity_rows(inverse_t, starts, count, me)
    whole = [parts[0] for parts in back[:-1]]
    out, at = None, 0
    for tail, number in zip(back[-1], cut_out[-1]):
        blocks = [block] * number
        if at + number * block == cells:
            blocks[-1:] = [LANES * n for n in cut(block // LANES, 2)]
        out = last_step(upper.reshape(1), weight, [*whole, tail], out, at, blocks, cells, width)
        at += number * block
    return out.reshape(field.shape)


def plain_body(count_i, count_k, field, forward, inverse, eigen):
    half = forward.shape[1]
    i_local, k_local, width = field.shape
    count = count_i * count_k
    rows = width // count
    high = lax.Precision.HIGHEST
    px, pz = lax.axis_index("px"), lax.axis_index("pz")
    me = lax.axis_index(AXES)
    eigen2 = eigen.reshape(2, half)
    x = jnp.einsum("pjm,ikpm->pjik", forward, field.reshape(i_local, k_local, 2, half), precision=high)
    x = lax.all_to_all(x.reshape(count, rows, i_local, k_local), AXES, split_axis=0, concat_axis=0, tiled=True)
    x = x.reshape(count_i, count_k, rows, i_local, k_local).transpose(2, 0, 3, 1, 4).reshape(rows, half, half)
    x = jnp.einsum("nk,jik->jin", forward[pz], x, precision=high)
    x = jnp.einsum("ni,jik->jnk", forward[px], x, precision=high)
    eig = lax.dynamic_slice_in_dim(eigen, me * rows, rows)
    x = x / (eigen2[px][None, :, None] + eigen2[pz][None, None, :] + eig[:, None, None])
    x = jnp.einsum("ni,jik->jnk", inverse[px], x, precision=high)
    x = jnp.einsum("nk,jik->jin", inverse[pz], x, precision=high)
    x = x.reshape(rows, count_i, i_local, count_k, k_local).transpose(1, 3, 0, 2, 4).reshape(count, rows, i_local, k_local)
    x = lax.all_to_all(x, AXES, split_axis=0, concat_axis=0, tiled=True)
    x = jnp.einsum("pjm,pmik->ikpj", inverse, x.reshape(2, half, i_local, k_local), precision=high)
    return x.reshape(field.shape)


def solution(mesh):
    gx, gy, gz = (mesh.shape[name] for name in ("gx", "gy", "gz"))
    parts = Mesh(mesh.devices.reshape(2, gx // 2, gy, 2, gz // 2), ("px", "xl", "gy", "pz", "zl"))
    count_i, count_k = gx // 2 * gy, gz // 2

    fast_mesh = count_k == 2 and count_i & (count_i - 1) == 0

    def body(field, forward, inverse, eigen):
        i_local, k_local, width = field.shape
        fast = (
            fast_mesh
            and k_local <= LANES
            and width == count_i * count_k * sum(chunk[0] for chunk in CHUNKS)
            and i_local * k_local % math.lcm(k_local, LANES) == 0
            and i_local * k_local > math.lcm(k_local, LANES)
        )
        if fast:
            return fast_body(count_i * count_k, field, forward, inverse, eigen)
        return plain_body(count_i, count_k, field, forward, inverse, eigen)

    spec = P(("px", "xl", "gy"), ("pz", "zl"), None)
    return jax.shard_map(body, mesh=parts, in_specs=(spec, P(), P(), P()), out_specs=spec, check_vma=False)
```

```python
import math

import jax
import jax.numpy as jnp
from jax import lax
from jax.experimental import pallas as pl
from jax.experimental.pallas import tpu as pltpu
from jax.sharding import Mesh, PartitionSpec as P


AXES = ("xl", "gy", "zl")
LANES = 128
CHUNKS = ((24, 0), (8, None), (24, 1))


def split(x):
    high = x.astype(jnp.bfloat16)
    low = (x - high.astype(jnp.float32)).astype(jnp.bfloat16)
    return high, low


def dot3(a, b, dims):
    ah, al = a
    bh, bl = b
    dot = lambda u, v: lax.dot_general(u, v, (dims, ((), ())), preferred_element_type=jnp.float32)
    return dot(ah, bh) + (dot(ah, bl) + dot(al, bh))


def cut(total, parts):
    sizes = []
    for left in range(parts, 0, -1):
        sizes.append(-(-(total - sum(sizes)) // left))
    return sizes


def sending_order(count):
    far = [d for d in range(2, count) if 2 * d >= count]
    near = [d for d in range(1, count) if d not in far]
    order = [0]
    for pair in zip([d for d in far if d % 2 == 0], [d for d in near if d % 2 == 1]):
        order += pair
    return order + [d for d in far + near if d not in order]


def shares(count, chunk):
    return [count // 2 if chunk[1] is None else count * (chunk[1] == p) for p in range(2)]


def swap_blocks(x, index, axis):
    count = x.shape[axis]
    bits = count.bit_length() - 1
    shape = x.shape
    x = x.reshape(shape[:axis] + (2,) * bits + shape[axis + 1:])
    for bit in range(bits):
        at = axis + bits - 1 - bit
        x = jnp.where((index >> bit) & 1 == 1, jnp.flip(x, at), x)
    return x.reshape(shape)


def pad_last(x, axis, to):
    widths = [(0, 0)] * x.ndim
    widths[axis] = (0, to - x.shape[axis])
    return jnp.pad(x, widths)


def load_field(field_ref, data, sems, start, block):
    step = pl.program_id(0)
    copies = data.shape[0] // block

    def copy(r):
        source = field_ref.at[pl.ds((start + r) * block, block), pl.ds(0, data.shape[1])]
        return pltpu.make_async_copy(source, data.at[pl.ds(r * block, block), :], sems.at[r])

    @pl.when(step == 0)
    def _():
        for r in range(copies):
            copy(r).start()

    copy(step).wait()
    return data[pl.ds(pl.multiple_of(step * block, 8), block), :]


def write_pieces(result, out_refs):
    rows = out_refs[0].shape[0]
    for d, out in zip(sending_order(len(out_refs)), out_refs):
        out[...] = result[d * rows:(d + 1) * rows]


def lead_kernel(count, start, block, me_ref, forward_ref, field_ref, _, *refs):
    outs, (data, sems, matrix, weight_sem) = refs[:count], refs[count:]
    half = forward_ref.shape[2]
    rows = outs[0].shape[0]
    get = pltpu.make_async_copy(forward_ref.at[0], matrix, weight_sem)

    @pl.when(pl.program_id(0) == 0)
    def _():
        get.start()

    values = load_field(field_ref, data, sems, start, block)[:, :half]

    @pl.when(pl.program_id(0) == 0)
    def _():
        get.wait()

    weight = jnp.concatenate([matrix[pl.ds(pl.multiple_of((me_ref[0] ^ d) * rows, 8), rows), :] for d in range(count)], axis=0)
    write_pieces(dot3(split(weight), split(values), ((1,), (1,))), outs)


def next_kernel(count, start, block, weight_ref, field_ref, _, *refs):
    outs, (data, sems) = refs[:count], refs[count:]
    values = load_field(field_ref, data, sems, start, block)
    write_pieces(dot3(split(weight_ref[...]), split(values), ((1,), (1,))), outs)


def first_step(kernel, operands, specs, scratch, field, after, rows, count, start, number, width, block):
    hbm = pl.BlockSpec(memory_space=pl.ANY)
    return pl.pallas_call(
        lambda *refs: kernel(count, start, block, *refs),
        grid=(number,),
        in_specs=[*specs, hbm, hbm],
        out_specs=[pl.BlockSpec((rows, block), lambda r: (0, r))] * count,
        out_shape=[jax.ShapeDtypeStruct((rows, number * block), jnp.float32)] * count,
        scratch_shapes=[pltpu.VMEM((number * block, width), jnp.float32), pltpu.SemaphoreType.DMA((number,)), *scratch],
        cost_estimate=pl.CostEstimate(flops=6 * number * block * width * rows * count, bytes_accessed=4 * number * block * (width + rows * count), transcendentals=0),
    )(*operands, field, after)


def middle_kernel(i_local, k_local, count, units_in, units, eig_ref, ek_ref, ei_ref, fk_ref, fi_ref, gi_ref, gk_ref, *refs):
    given = count * len(units_in)
    ins, outs, work = refs[:given], refs[given:-2], refs[-2:]
    rows = ins[0].shape[0]
    place = [sending_order(count).index(d) for d in range(count)]
    i_blocks = count // 2
    period = math.lcm(k_local, LANES)
    i_per, tiles = period // k_local, period // LANES
    lane = lax.broadcasted_iota(jnp.int32, (rows, LANES), 1)

    for dy in range(i_blocks):
        begin = 0
        for s, number in enumerate(units_in):
            def spread(g, _, dy=dy, s=s, begin=begin):
                base = pl.multiple_of(g * period, LANES)
                for half in range(2):
                    ref = ins[s * count + place[2 * dy + half]]
                    data = [ref[:, pl.ds(base + LANES * q, LANES)] for q in range(tiles)]
                    for t in range(i_per):
                        q, off = divmod(t * k_local, LANES)
                        x = data[q]
                        if off + k_local > LANES:
                            x = jnp.where(lane >= off, x, data[q + 1])
                        if off:
                            x = pltpu.roll(x, LANES - off, 1)
                        at = pl.multiple_of((dy * i_local + (begin + g) * i_per + t) * rows, 8)
                        work[half][pl.ds(at, rows), :] = x
                return 0

            lax.fori_loop(0, number, spread, 0)
            begin += number

    fk, fi, gi, gk = split(fk_ref[...]), split(fi_ref[...]), split(gi_ref[...]), split(gk_ref[...])
    size = i_blocks * i_local
    eigen_ik = ei_ref[...] + ek_ref[...]

    def solve(j, _):
        x = jnp.concatenate([ref[pl.ds(j, size, stride=rows), :] for ref in work], axis=1)
        x = dot3(split(x), fk, ((1,), (0,)))
        x = dot3(fi, split(x), ((1,), (0,)))
        x = x / (eigen_ik + eig_ref[0, j])
        x = dot3(gi, split(x), ((1,), (0,)))
        x = dot3(split(x), gk, ((1,), (0,)))
        for half, ref in enumerate(work):
            ref[pl.ds(j, size, stride=rows), :] = x[:, half * LANES:(half + 1) * LANES]
        return 0

    lax.fori_loop(0, rows, solve, 0)

    for dy in range(i_blocks):
        begin = 0
        for s, number in enumerate(units):
            def gather(g, _, dy=dy, s=s, begin=begin):
                base = pl.multiple_of(g * period, LANES)
                for half in range(2):
                    data = []
                    for t in range(i_per):
                        at = pl.multiple_of((dy * i_local + (begin + g) * i_per + t) * rows, 8)
                        data.append(work[half][pl.ds(at, rows), :])
                    for q in range(tiles):
                        t, off = divmod(q * LANES, k_local)
                        left = k_local - off
                        x = pltpu.roll(data[t], LANES - off, 1) if off else data[t]
                        if left < LANES:
                            x = jnp.where(lane < left, x, pltpu.roll(data[t + 1], left, 1))
                        outs[s * count + place[2 * dy + half]][:, pl.ds(base + LANES * q, LANES)] = x
                return 0

            lax.fori_loop(0, number, gather, 0)
            begin += number


def middle_step(sent, eig, ek, ei, fk, fi, gi, gk, i_local, k_local, units_in, units):
    count = len(sent[0])
    rows = sent[0][0].shape[0]
    cells = i_local * k_local
    size = count // 2 * i_local
    vmem = pl.BlockSpec(memory_space=pltpu.VMEM)
    unit = cells // sum(units)
    pieces = [piece for part in sent for piece in part]
    outs = pl.pallas_call(
        lambda *refs: middle_kernel(i_local, k_local, count, units_in, units, *refs),
        in_specs=[pl.BlockSpec(memory_space=pltpu.SMEM)] + [vmem] * (6 + len(pieces)),
        out_specs=[vmem] * (count * len(units)),
        out_shape=[jax.ShapeDtypeStruct((rows, n * unit), jnp.float32) for n in units for _ in range(count)],
        scratch_shapes=[pltpu.VMEM((size * rows, LANES), jnp.float32)] * 2,
        cost_estimate=pl.CostEstimate(flops=4 * 6 * rows * size * 256 * 256, bytes_accessed=8 * rows * cells * count, transcendentals=0),
        name="middle",
    )(eig, ek, ei, fk, fi, gi, gk, *pieces)
    return [outs[s * count:(s + 1) * count] for s in range(len(units))]


def last_kernel(count, start, blocks, upper_ref, weight_ref, *refs):
    total = count * len(CHUNKS)
    pieces = refs[-6 - total:-6]
    out_ref, stage, result, matrix, in_sems, out_sems = refs[-6:]
    half = weight_ref.shape[2]
    get = pltpu.make_async_copy(weight_ref, matrix, out_sems.at[len(blocks)])
    get.start()

    def copies(b, at, size):
        found, row = [], 0
        for n, piece in enumerate(pieces):
            rows = piece.shape[0]
            base = start if n < total - count else 0
            to = row + sending_order(count)[n % count] * rows
            found.append(pltpu.make_async_copy(piece.at[:, pl.ds(base + at, size)], stage.at[pl.ds(to, rows), pl.ds(at, size)], in_sems.at[b, n]))
            if n % count == count - 1:
                row += count * rows
        return found

    def put(b, at, size):
        return pltpu.make_async_copy(result.at[pl.ds(at, size), :], out_ref.at[pl.ds(start + at, size), :], out_sems.at[b])

    spans = [(b, sum(blocks[:b]), size) for b, size in enumerate(blocks)]
    for span in spans:
        for copy in copies(*span):
            copy.start()
    get.wait()
    weights = [split(matrix[p]) for p in range(2)]
    for b, at, size in spans:
        for copy in copies(b, at, size):
            copy.wait()
        for p in range(2):
            parts, row = [], 0
            for chunk in CHUNKS:
                rows = shares(count, chunk)[p] * chunk[0]
                if chunk[1] is None:
                    parts.append(stage[pl.ds(pl.multiple_of(row + (upper_ref[0] ^ p) * rows, 8), rows), at:at + size])
                elif rows:
                    parts.append(stage[row:row + rows, at:at + size])
                row += count * chunk[0]
            values = split(jnp.concatenate(parts, axis=0))
            result[at:at + size, p * half:(p + 1) * half] = dot3(values, weights[p], ((0,), (0,)))
        put(b, at, size).start()
    for span in spans:
        put(*span).wait()


def last_step(upper, weight, chunks, out, start, blocks, cells, width):
    pieces = [piece for chunk in chunks for piece in chunk]
    before = [] if out is None else [out]
    operands = [upper, weight, *before, *pieces]
    hbm = pl.BlockSpec(memory_space=pl.ANY)
    specs = [pl.BlockSpec(memory_space=pltpu.SMEM)] + [hbm] * (len(operands) - 1)
    aliases = {2: 0} if before else {}
    lanes = sum(blocks)
    return pl.pallas_call(
        lambda *refs: last_kernel(len(chunks[0]), start, blocks, *refs),
        in_specs=specs,
        out_specs=hbm,
        out_shape=jax.ShapeDtypeStruct((cells, width), jnp.float32),
        input_output_aliases=aliases,
        scratch_shapes=[
            pltpu.VMEM((sum(piece.shape[0] for piece in pieces), lanes), jnp.float32),
            pltpu.VMEM((lanes, width), jnp.float32),
            pltpu.VMEM(weight.shape, jnp.float32),
            pltpu.SemaphoreType.DMA((len(blocks), len(pieces))),
            pltpu.SemaphoreType.DMA((len(blocks) + 1,)),
        ],
        cost_estimate=pl.CostEstimate(flops=6 * lanes * weight.size, bytes_accessed=8 * lanes * width, transcendentals=0),
        name="last",
    )(*operands)


def block_rows(matrix, chunk, starts, count, me):
    half = matrix.shape[1]
    parts = []
    for p, share in enumerate(shares(count, chunk)):
        if share:
            rows = matrix[p, starts[p]:starts[p] + share * chunk[0]]
            parts.append(jnp.pad(rows, ((0, 0), (p * half, (1 - p) * half))))
    rows = jnp.concatenate(parts, axis=0).reshape(count, chunk[0], 2 * half)
    return swap_blocks(rows, me, 0).reshape(-1, 2 * half)


def parity_rows(matrix, starts, count, me):
    sides = []
    for p in range(2):
        parts = []
        for chunk, start in zip(CHUNKS, starts):
            share = shares(count, chunk)[p]
            if share:
                rows = matrix[p, start[p]:start[p] + share * chunk[0]].reshape(share, chunk[0], -1)
                parts.append(swap_blocks(rows, me % share, 0).reshape(share * chunk[0], -1))
        sides.append(jnp.concatenate(parts, axis=0))
    return jnp.stack(sides)


def fast_body(count, field, forward, inverse, eigen):
    half = forward.shape[1]
    i_local, k_local, width = field.shape
    cells = i_local * k_local
    i_blocks = count // 2
    px, pz = lax.axis_index("px"), lax.axis_index("pz")
    me = lax.axis_index(AXES)
    me_l, me_i, upper = me % 2, me // 2, me // (count // 2)
    flat = field.reshape(cells, width)
    block = math.lcm(k_local, LANES)
    total = cells // block

    starts, at = [], (0, 0)
    for chunk in CHUNKS:
        starts.append(at)
        at = tuple(a + n * chunk[0] for a, n in zip(at, shares(count, chunk)))

    order = sending_order(count)

    def exchange(pieces):
        moved = [pieces[0]]
        for d, piece in zip(order[1:], pieces[1:]):
            moved.append(lax.ppermute(piece, AXES, [(s, s ^ d) for s in range(count)]))
        return moved

    vmem, smem, hbm = (pl.BlockSpec(memory_space=space) for space in (pltpu.VMEM, pltpu.SMEM, pl.ANY))
    scratch = [pltpu.VMEM((half, half), jnp.float32), pltpu.SemaphoreType.DMA]
    lead_width = -(-half // LANES) * LANES
    cut_in = [[total // 2, total - total // 2]] + [[total]] * (len(CHUNKS) - 1)
    cut_out = [[total]] * (len(CHUNKS) - 1) + [[total - 3, 2, 1]]
    sent = [[]]
    after, start = flat, 0
    for number in cut_in[0]:
        pieces = first_step(lead_kernel, (me.reshape(1), forward), [smem, hbm], scratch, flat, after, CHUNKS[0][0], count, start, number, lead_width, block)
        sent[0].append(exchange(pieces))
        after = pieces[0]
        start += number
    forward, inverse, eigen, _ = lax.optimization_barrier((forward, inverse, eigen, after))
    for chunk, start in zip(CHUNKS[1:], starts[1:]):
        weight = block_rows(forward, chunk, start, count, me)
        pieces = first_step(next_kernel, (weight,), [vmem], [], flat, after, chunk[0], count, 0, total, width, block)
        sent.append([exchange(pieces)])
        after = pieces[0]

    eigen2 = eigen.reshape(2, half)
    inverse_t = inverse.transpose(0, 2, 1)
    fk = swap_blocks(forward[pz].T.reshape(2, k_local, half), me_l, 0)
    fk = pad_last(fk, 1, LANES).reshape(2 * LANES, 2, k_local)
    fk = pad_last(fk, 2, LANES).reshape(2 * LANES, 2 * LANES)
    gk = swap_blocks(inverse_t[pz].reshape(half, 2, k_local), me_l, 1)
    gk = pad_last(gk, 2, LANES).reshape(2, k_local, 2 * LANES)
    gk = pad_last(gk, 1, LANES).reshape(2 * LANES, 2 * LANES)
    fi = swap_blocks(forward[px].reshape(half, i_blocks, i_local), me_i, 1).reshape(half, half)
    gi = swap_blocks(inverse[px].reshape(i_blocks, i_local, half), me_i, 0).reshape(half, half)
    ek = jnp.pad(eigen2[pz].reshape(2, k_local), ((0, 0), (0, LANES - k_local)), constant_values=1.0).reshape(1, 2 * LANES)
    ei = eigen2[px].reshape(half, 1)

    back = []
    for chunk, start, parts, units_in, units in zip(CHUNKS, starts, sent, cut_in, cut_out):
        if chunk[1] is None:
            own = upper * half + jnp.where(upper == 1, start[1], start[0]) + me % (count // 2) * chunk[0]
        else:
            own = chunk[1] * half + start[chunk[1]] + me * chunk[0]
        eig = lax.dynamic_slice_in_dim(eigen, own, chunk[0]).reshape(1, -1)
        if back:
            eig, _ = lax.optimization_barrier((eig, back[-1][0][0]))
        done = middle_step(parts, eig, ek, ei, fk, fi, gi, gk, i_local, k_local, units_in, units)
        back.append([exchange(part) for part in done])
    weight = parity_rows(inverse_t, starts, count, me)
    whole = [parts[0] for parts in back[:-1]]
    out, at = None, 0
    for tail, number in zip(back[-1], cut_out[-1]):
        blocks = [block] * number
        if at + number * block == cells:
            blocks[-1:] = [LANES * n for n in cut(block // LANES, 2)]
        out = last_step(upper.reshape(1), weight, [*whole, tail], out, at, blocks, cells, width)
        at += number * block
    return out.reshape(field.shape)


def plain_body(count_i, count_k, field, forward, inverse, eigen):
    half = forward.shape[1]
    i_local, k_local, width = field.shape
    count = count_i * count_k
    rows = width // count
    high = lax.Precision.HIGHEST
    px, pz = lax.axis_index("px"), lax.axis_index("pz")
    me = lax.axis_index(AXES)
    eigen2 = eigen.reshape(2, half)
    x = jnp.einsum("pjm,ikpm->pjik", forward, field.reshape(i_local, k_local, 2, half), precision=high)
    x = lax.all_to_all(x.reshape(count, rows, i_local, k_local), AXES, split_axis=0, concat_axis=0, tiled=True)
    x = x.reshape(count_i, count_k, rows, i_local, k_local).transpose(2, 0, 3, 1, 4).reshape(rows, half, half)
    x = jnp.einsum("nk,jik->jin", forward[pz], x, precision=high)
    x = jnp.einsum("ni,jik->jnk", forward[px], x, precision=high)
    eig = lax.dynamic_slice_in_dim(eigen, me * rows, rows)
    x = x / (eigen2[px][None, :, None] + eigen2[pz][None, None, :] + eig[:, None, None])
    x = jnp.einsum("ni,jik->jnk", inverse[px], x, precision=high)
    x = jnp.einsum("nk,jik->jin", inverse[pz], x, precision=high)
    x = x.reshape(rows, count_i, i_local, count_k, k_local).transpose(1, 3, 0, 2, 4).reshape(count, rows, i_local, k_local)
    x = lax.all_to_all(x, AXES, split_axis=0, concat_axis=0, tiled=True)
    x = jnp.einsum("pjm,pmik->ikpj", inverse, x.reshape(2, half, i_local, k_local), precision=high)
    return x.reshape(field.shape)


def solution(mesh):
    gx, gy, gz = (mesh.shape[name] for name in ("gx", "gy", "gz"))
    parts = Mesh(mesh.devices.reshape(2, gx // 2, gy, 2, gz // 2), ("px", "xl", "gy", "pz", "zl"))
    count_i, count_k = gx // 2 * gy, gz // 2

    fast_mesh = count_k == 2 and count_i & (count_i - 1) == 0

    def body(field, forward, inverse, eigen):
        i_local, k_local, width = field.shape
        fast = (
            fast_mesh
            and k_local <= LANES
            and width == count_i * count_k * sum(chunk[0] for chunk in CHUNKS)
            and i_local * k_local % math.lcm(k_local, LANES) == 0
            and i_local * k_local >= 4 * math.lcm(k_local, LANES)
        )
        if fast:
            return fast_body(count_i * count_k, field, forward, inverse, eigen)
        return plain_body(count_i, count_k, field, forward, inverse, eigen)

    spec = P(("px", "xl", "gy"), ("pz", "zl"), None)
    return jax.shard_map(body, mesh=parts, in_specs=(spec, P(), P(), P()), out_specs=spec, check_vma=False)
```
